512 devices in a mesh: inst: 16 (over x, z_hi, core), shard: 32 (over y, z_lo).
Axes of the slice: x: 4, y: 4, z: 16 (z_hi: 2, z_lo: 8; z = z_hi * 8 + z_lo), core: 2. Of those that a mesh axis runs over, the one named last changes fastest.
Arguments:
- tokens: bfloat16 [32768, 5120], P(('inst', 'shard')), may hold values from -600 to 600
- norm_gain: float32 [5120], P(('inst', 'shard')), may hold values from 0.1 to 1.9
- master_qkv: float32 [5120, 7168], P(('inst', 'shard')), may hold values from -0.078125 to 0.078125
- qkv_bias: float32 [7168], P(('inst', 'shard')), may hold values from -3 to 3
Outputs:
- qkv_out: bfloat16 [512, 512, 896], P(('inst', 'shard'))
The draws below stay inside these ranges and needn't reach their ends.
All inputs are finite; a program needn't handle non-finite values.
Results may differ from the reference program's by a relative error of at most 0.0062.
Values may be sent and summed in bfloat16 or wider, within the bound.
No kernel may reach another device: no remote copies, remote signals or barrier semaphores. Data moves between devices by JAX's collectives and lax.ppermute only.
A program may use at most 64 MiB of HBM per device.

```python
import jax
import jax.numpy as jnp
from jax import lax

D = 5120
QHEADS = 40
KVHEADS = 8
HEAD_DIM = 128
TP = 8
TOK_DEV = 64
QKVW = 7168
TOKENS = 32768
N_INST = 16
N_SHARD = 32


def draw_tokens(key, part):
    row_key, col_key, base_key = jax.random.split(key, 3)
    base = jax.random.truncated_normal(base_key, -4.0, 4.0, (TOKENS, D), jnp.float32)
    row_scale = jnp.power(10.0, jax.random.uniform(row_key, (TOKENS, 1), jnp.float32, 0.0, 1.0))
    col_scale = jnp.power(10.0, jax.random.uniform(col_key, (1, D), jnp.float32, 0.0, 1.0))
    return (base * row_scale * col_scale).astype(jnp.bfloat16)


def block_scale(stream_key, shape, cuts, smallest, largest):
    level = 1.0
    for position, shards_of in cuts:
        heights = jax.random.uniform(jax.random.fold_in(jax.random.fold_in(stream_key, 6), position), (shards_of,), jnp.float32, smallest / len(cuts), largest / len(cuts))
        level = level * jnp.repeat(jnp.exp(heights), shape[position] // shards_of).reshape((-1,) + (1,) * (len(shape) - 1 - position))
    return level


def scatter_about(stream_key, extent, scale, bound, cuts=(), dtype=jnp.bfloat16):
    entries = jax.random.normal(stream_key, extent, jnp.float32) * scale
    if len(cuts) > 0:
        entries = block_scale(stream_key, extent, cuts, -0.22, 0.18) * entries
    return jnp.clip(entries, min=-bound, max=bound).astype(dtype)


def setup_inputs(seed: int = 0) -> dict:
    key_of = jax.random.split(jax.random.key(seed), 5)
    tokens = draw_tokens(jax.random.fold_in(key_of[4], 71), 0)
    norm_gain = jnp.clip(1.0 + 0.18 * jax.random.normal(key_of[1], (D,), jnp.float32), 0.1, 1.9)
    master_qkv = scatter_about(key_of[2], (D, QKVW), D ** -0.5, 0.078125, ((0, 512),), jnp.float32)
    qkv_bias = scatter_about(key_of[3], (QKVW,), 0.5, 3.0, ((0, 512),), jnp.float32)
    return {"tokens": tokens, "norm_gain": norm_gain, "master_qkv": master_qkv, "qkv_bias": qkv_bias}


EPSILON = 1e-06

def rank_columns(matrix):
    query_cols = QHEADS * HEAD_DIM
    pair_cols = KVHEADS * HEAD_DIM
    leading = matrix.shape[:-1]
    query = matrix[..., :query_cols].reshape(leading + (TP, query_cols // TP))
    keys = matrix[..., query_cols:query_cols + pair_cols].reshape(leading + (TP, pair_cols // TP))
    values = matrix[..., query_cols + pair_cols:].reshape(leading + (TP, pair_cols // TP))
    return jnp.concatenate([query, keys, values], axis=-1)

def normalize(tokens, gain):
    floats = tokens.astype(jnp.float32)
    scale = lax.rsqrt(lax.optimization_barrier(jnp.mean(floats * floats, axis=-1, keepdims=True)) + EPSILON)
    return (floats * scale * gain.astype(jnp.float32)).astype(jnp.bfloat16)

def reference(tokens, norm_gain, master_qkv, qkv_bias):
    weights = master_qkv.astype(jnp.bfloat16)
    gain_low = norm_gain.astype(jnp.bfloat16)
    bias_low = qkv_bias.astype(jnp.bfloat16)
    normed = normalize(tokens, gain_low)
    rank_width = QKVW // TP
    flat_weights = rank_columns(weights).reshape(D, TP * rank_width)
    flat_bias = rank_columns(bias_low).reshape(TP * rank_width).astype(jnp.float32)
    group_tokens = TP * TOK_DEV
    groups = normed.reshape(TOKENS // group_tokens, group_tokens, D)

    def project(group_rows):
        product = jnp.dot(group_rows, flat_weights, preferred_element_type=jnp.float32) + flat_bias
        shaped = product.astype(jnp.bfloat16).reshape(group_tokens, TP, rank_width)
        return jnp.transpose(shaped, (1, 0, 2))
    outputs = lax.map(project, groups)
    return outputs.reshape(N_INST * N_SHARD, group_tokens, rank_width)
```

```python
import jax
import jax.numpy as jnp
from jax import lax
from jax.sharding import Mesh
from jax.sharding import PartitionSpec as P

QHEADS = 40
KVHEADS = 8
HEAD_DIM = 128
TP = 8
EPSILON = 1e-06

ZLINE = ("zhi", "zlo")
PLANE = ("x", "core", "y")
ALL = ("x", "zhi", "core", "y", "zlo")


def rank_columns(matrix):
    query_cols = QHEADS * HEAD_DIM
    pair_cols = KVHEADS * HEAD_DIM
    leading = matrix.shape[:-1]
    query = matrix[..., :query_cols].reshape(leading + (TP, query_cols // TP))
    keys = matrix[..., query_cols : query_cols + pair_cols].reshape(leading + (TP, pair_cols // TP))
    values = matrix[..., query_cols + pair_cols :].reshape(leading + (TP, pair_cols // TP))
    return jnp.concatenate([query, keys, values], axis=-1)


def per_device(tokens, norm_gain, master_qkv, qkv_bias):
    local_rows, width = master_qkv.shape
    rank_width = width // TP
    token_rows, depth = tokens.shape
    floats = tokens.astype(jnp.float32)
    scale = lax.rsqrt(jnp.mean(floats * floats, axis=-1, keepdims=True) + EPSILON)
    normed = (floats * scale).astype(jnp.bfloat16)
    group_rows = lax.all_gather(normed, "zlo", axis=0, tiled=True)

    gain = norm_gain.astype(jnp.bfloat16).astype(jnp.float32)[:, None]
    rows = (gain * master_qkv.astype(jnp.bfloat16).astype(jnp.float32)).astype(jnp.bfloat16)
    device = lax.axis_index(ALL)
    bias_row = lax.dynamic_update_slice(
        jnp.zeros((width,), jnp.bfloat16), qkv_bias.astype(jnp.bfloat16), (device * qkv_bias.shape[0],)
    )
    rows = jnp.concatenate([rows, bias_row[None]], axis=0)
    ranked = jnp.transpose(rank_columns(rows), (1, 0, 2))
    outgoing = jnp.concatenate([ranked, ranked], axis=0)
    arrived = lax.all_to_all(outgoing, ZLINE, split_axis=0, concat_axis=0, tiled=True)
    weight_part = arrived[:, :local_rows].reshape(16 * local_rows, rank_width)
    bias_part = jnp.sum(arrived[:, local_rows].astype(jnp.float32), axis=0).astype(jnp.bfloat16)
    bias_part = jnp.pad(bias_part[None], ((0, 7), (0, 0)))
    sent = jnp.concatenate([weight_part, bias_part], axis=0)
    planes = lax.all_gather(sent, PLANE, axis=0, tiled=False)
    bias_mine = jnp.sum(planes[:, 16 * local_rows].astype(jnp.float32), axis=0)
    weights = planes[:, : 16 * local_rows].reshape(4, 8, 2, 8 * local_rows, rank_width)
    weights = jnp.transpose(weights, (0, 2, 1, 3, 4)).reshape(depth, rank_width)
    product = jnp.dot(group_rows, weights, preferred_element_type=jnp.float32)
    return (product + bias_mine).astype(jnp.bfloat16)[None]


def solution(mesh):
    fine = Mesh(mesh.devices.reshape(4, 2, 2, 4, 8), ALL)
    in_specs = (P(ALL, None), P(ALL), P(ALL, None), P(ALL))
    return jax.shard_map(
        per_device, mesh=fine, in_specs=in_specs, out_specs=P(ALL, None, None), check_vma=False
    )
```

```python
import functools

import jax
import jax.numpy as jnp
from jax import lax
from jax.experimental import pallas as pl
from jax.experimental.pallas import tpu as pltpu
from jax.sharding import Mesh
from jax.sharding import PartitionSpec as P


QHEADS = 40
KVHEADS = 8
TP = 8
EPSILON = 1e-06

ZLINE = ("zhi", "zlo")
PLANE = ("x", "core", "y")
ALL = ("x", "zhi", "core", "y", "zlo")
NX, NZHI, NCORE, NY, NZLO = 4, 2, 2, 4, 8
NZ = NZHI * NZLO
LANES = 128
EARLY = 4
MIB = 1 << 20


def rank_tiles():
    q = QHEADS // TP
    return [
        [r * q + c for c in range(q)] + [QHEADS + r, QHEADS + KVHEADS + r] for r in range(TP)
    ]


def pack_kernel(master_ref, gain_ref, bias_ref, out_ref, line):
    rows = master_ref.shape[0]
    gain = gain_ref[...].astype(jnp.bfloat16).astype(jnp.float32)
    for r, tiles in enumerate(rank_tiles()):
        line[...] = jnp.zeros_like(line)
        for c, t in enumerate(tiles):
            piece = master_ref[:, t * LANES : (t + 1) * LANES]
            line[c * rows : (c + 1) * rows, :] = gain * piece.astype(jnp.bfloat16).astype(jnp.float32)
            at = len(tiles) * rows + c
            line[at : at + 1, :] = bias_ref[t : t + 1, :]
        block = line[...].astype(jnp.bfloat16)
        for h in range(NZHI):
            out_ref[h * TP + r] = block


def pack(master, gain, bias_row):
    rows = master.shape[0]
    return pl.pallas_call(
        pack_kernel,
        out_shape=jax.ShapeDtypeStruct((NZ, 80, LANES), jnp.bfloat16),
        scratch_shapes=[pltpu.VMEM((80, LANES), jnp.float32)],
        compiler_params=pltpu.CompilerParams(vmem_limit_bytes=8 * MIB),
        name="pack",
    )(master, gain.reshape(rows, 1), bias_row)


def unpack_kernel(rows, lines_ref, out_ref, line, wide):
    tiles = wide.shape[1] // LANES
    total = jnp.zeros((8, LANES), jnp.float32)
    for s in range(NZ):
        line[...] = lines_ref[s].astype(jnp.float32)
        for c in range(tiles):
            wide[s * rows : (s + 1) * rows, c * LANES : (c + 1) * LANES] = line[c * rows : (c + 1) * rows, :]
        total = total + line[tiles * rows : tiles * rows + 8, :]
    line[0:8, :] = total
    wide[NZ * rows :, :] = jnp.zeros((8, wide.shape[1]), jnp.float32)
    for c in range(tiles):
        wide[NZ * rows : NZ * rows + 1, c * LANES : (c + 1) * LANES] = line[c : c + 1, :]
    out_ref[...] = wide[...].astype(jnp.bfloat16)


def unpack(lines, rows, width):
    high = NZ * rows + 8
    return pl.pallas_call(
        functools.partial(unpack_kernel, rows),
        out_shape=jax.ShapeDtypeStruct((high, width), jnp.bfloat16),
        scratch_shapes=[pltpu.VMEM((80, LANES), jnp.float32), pltpu.VMEM((high, width), jnp.float32)],
        compiler_params=pltpu.CompilerParams(vmem_limit_bytes=8 * MIB),
        name="unpack",
    )(lines)


def start_weights(planes, wbuf, bbuf, wsem, bsem, run):
    depth = wbuf.shape[0]
    chunk = depth // NX
    for x in range(NX):
        for h in range(NZHI):
            for c in range(NCORE):
                for y in range(NY):
                    at = (((x * NZHI + h) * NCORE + c) * NY + y) * run
                    pltpu.make_async_copy(
                        planes.at[(x * NCORE + c) * NY + y, h * run : (h + 1) * run],
                        wbuf.at[at : at + run],
                        wsem.at[x],
                    ).start()
    bias_copy = pltpu.make_async_copy(planes.at[:, NZHI * run : NZHI * run + 8], bbuf, bsem)
    bias_copy.start()
    return chunk, bias_copy


def multiply(x, wbuf, bbuf, acc, wsem, bias_copy, chunk):
    def step(i, _):
        here = pl.ds(pl.multiple_of(i * chunk, chunk), chunk)
        pltpu.make_async_copy(wbuf.at[here], wbuf.at[here], wsem.at[i]).wait()
        part = jnp.dot(x[:, here], wbuf[here, :], preferred_element_type=jnp.float32)

        @pl.when(i == 0)
        def _():
            acc[...] = part

        @pl.when(i > 0)
        def _():
            acc[...] += part

        return 0

    lax.fori_loop(0, NX, step, 0)
    bias_copy.wait()
    bias = jnp.sum(jnp.sum(bbuf[...].astype(jnp.float32), axis=0), axis=0, keepdims=True)
    return (acc[...] + bias).astype(jnp.bfloat16)


def token_copies(slots, x, sems, half):
    copies = []
    for i, (refs, cond, row) in enumerate(slots):
        for h, ref in enumerate(refs):
            at = pl.multiple_of(row + h * half, 8)
            copies.append((cond, pltpu.make_async_copy(ref, x.at[pl.ds(at, half)], sems.at[2 * i + h])))
    return copies


def start_all(copies):
    for cond, copy in copies:
        pl.when(cond)(copy.start)


def wait_all(copies):
    for cond, copy in copies:
        pl.when(cond)(copy.wait)


def early_kernel(half, run, *refs):
    planes = refs[0]
    own = refs[1:3]
    left = [refs[3 + 2 * s : 5 + 2 * s] for s in range(EARLY)]
    right = [refs[3 + 2 * EARLY + 2 * s : 5 + 2 * EARLY + 2 * s] for s in range(EARLY)]
    out_ref, x, wbuf, bbuf, acc, wsem, bsem, xsem = refs[3 + 4 * EARLY :]
    me = lax.axis_index("zlo")
    chunk, bias_copy = start_weights(planes, wbuf, bbuf, wsem, bsem, run)
    block = 2 * half
    slots = [(own, me >= 0, me * block)]
    for s in range(1, EARLY + 1):
        slots.append((left[s - 1], me >= s, jnp.maximum(me - s, 0) * block))
        slots.append((right[s - 1], me + s < NZLO, jnp.minimum(me + s, NZLO - 1) * block))
    copies = token_copies(slots, x, xsem, half)
    start_all(copies)
    wait_all(copies)
    out_ref[...] = multiply(x, wbuf, bbuf, acc, wsem, bias_copy, chunk)


def late_kernel(half, run, *refs):
    late = NZLO - 1 - EARLY
    planes = refs[0]
    left = [refs[1 + 2 * s : 3 + 2 * s] for s in range(late)]
    right = [refs[1 + 2 * late + 2 * s : 3 + 2 * late + 2 * s] for s in range(late)]
    _, out_ref, x, wbuf, bbuf, acc, obuf, wsem, bsem, xsem, osem = refs[1 + 4 * late :]
    me = lax.axis_index("zlo")
    chunk, bias_copy = start_weights(planes, wbuf, bbuf, wsem, bsem, run)
    block = 2 * half
    copies = []
    for s in range(late):
        dist = EARLY + 1 + s
        copies += token_copies(
            [(left[s], me >= dist, s * block), (right[s], me + dist < NZLO, s * block)],
            x, xsem.at[s], half,
        )
    start_all(copies)
    wait_all(copies)
    obuf[...] = multiply(x, wbuf, bbuf, acc, wsem, bias_copy, chunk)
    outs = []
    for s in range(late):
        dist = EARLY + 1 + s
        go_left, go_right = me >= dist, me + dist < NZLO
        place = jnp.clip(jnp.where(go_left, me - dist, me + dist), 0, NZLO - 1)
        copy = pltpu.make_async_copy(
            obuf.at[s * block : (s + 1) * block],
            out_ref.at[pl.ds(pl.multiple_of(place * block, block), block)],
            osem.at[s],
        )
        outs.append((jnp.logical_or(go_left, go_right), copy))
    start_all(outs)
    wait_all(outs)


def common_scratch(rows, depth, width):
    return [
        pltpu.VMEM((rows, depth), jnp.bfloat16),
        pltpu.VMEM((depth, width), jnp.bfloat16),
        pltpu.VMEM((NX * NCORE * NY, 8, width), jnp.bfloat16),
        pltpu.VMEM((rows, width), jnp.float32),
    ]


def early_call(planes, own, left, right, run):
    half, depth = own[0].shape
    width = planes.shape[-1]
    rows = 2 * half * NZLO
    flat = [a for pair in [own] + left + right for a in pair]
    return pl.pallas_call(
        functools.partial(early_kernel, half, run),
        out_shape=jax.ShapeDtypeStruct((rows, width), jnp.bfloat16),
        in_specs=[pl.BlockSpec(memory_space=pltpu.HBM)] * (1 + len(flat)),
        scratch_shapes=common_scratch(rows, depth, width) + [
            pltpu.SemaphoreType.DMA((NX,)),
            pltpu.SemaphoreType.DMA,
            pltpu.SemaphoreType.DMA((2 * (1 + 2 * EARLY),)),
        ],
        compiler_params=pltpu.CompilerParams(vmem_limit_bytes=26 * MIB),
        cost_estimate=pl.CostEstimate(flops=2 * rows * depth * width, bytes_accessed=2 * depth * width, transcendentals=0),
        name="early",
    )(planes, *flat)


def late_call(planes, left, right, before, run):
    half, depth = left[0][0].shape
    width = planes.shape[-1]
    late = len(left)
    rows = 2 * half * late
    flat = [a for pair in left + right for a in pair]
    return pl.pallas_call(
        functools.partial(late_kernel, half, run),
        out_shape=jax.ShapeDtypeStruct(before.shape, jnp.bfloat16),
        in_specs=[pl.BlockSpec(memory_space=pltpu.HBM)] + [pl.BlockSpec(memory_space=pl.ANY)] * (1 + len(flat)),
        out_specs=pl.BlockSpec(memory_space=pl.ANY),
        input_output_aliases={1 + len(flat): 0},
        scratch_shapes=common_scratch(rows, depth, width) + [
            pltpu.VMEM((rows, width), jnp.bfloat16),
            pltpu.SemaphoreType.DMA((NX,)),
            pltpu.SemaphoreType.DMA,
            pltpu.SemaphoreType.DMA((late, 4)),
            pltpu.SemaphoreType.DMA((late,)),
        ],
        compiler_params=pltpu.CompilerParams(vmem_limit_bytes=20 * MIB),
        cost_estimate=pl.CostEstimate(flops=2 * rows * depth * width, bytes_accessed=2 * depth * width, transcendentals=0),
        name="late",
    )(planes, *flat, before)


def project(tokens, norm_gain, master_qkv, qkv_bias):
    local_rows, width = master_qkv.shape
    rank_width = width // TP
    token_rows, _ = tokens.shape
    half = token_rows // 2
    floats = tokens.astype(jnp.float32)
    scale = lax.rsqrt(jnp.mean(floats * floats, axis=-1, keepdims=True) + EPSILON)
    normed = (floats * scale).astype(jnp.bfloat16)
    own = [normed[:half], normed[half:]]

    to_right, to_left = [own], [own]
    for s in range(1, NZLO):
      up = [(k, k + 1) for k in range(s - 1, NZLO - 1)]
      down = [(k, k - 1) for k in range(1, NZLO - s + 1)]
      moved_right, moved_left = [], []
      for h in range(2):
          moved_right.append(lax.ppermute(to_right[-1][h], "zlo", up))
          moved_left.append(lax.ppermute(to_left[-1][h], "zlo", down))
      to_right.append(moved_right)
      to_left.append(moved_left)
    from_left, from_right = to_right[1:], to_left[1:]

    device = lax.axis_index(ALL)
    bias_row = lax.dynamic_update_slice(
        jnp.zeros((width,), jnp.float32),
        qkv_bias.astype(jnp.bfloat16).astype(jnp.float32),
        (device * qkv_bias.shape[0],),
    ).reshape(width // LANES, LANES)
    master_qkv, own[0], own[1] = lax.optimization_barrier((master_qkv, own[0], own[1]))
    lines = pack(master_qkv, norm_gain, bias_row)
    arrived = lax.all_to_all(lines, ZLINE, split_axis=0, concat_axis=0, tiled=True)
    block = unpack(arrived, local_rows, rank_width)
    planes = lax.all_gather(block, PLANE, axis=0, tiled=False)

    run = NZLO * local_rows
    first = early_call(planes, own, from_left[:EARLY], from_right[:EARLY], run)
    result = late_call(planes, from_left[EARLY:], from_right[EARLY:], first, run)
    return result[None]


def solution(mesh):
    fine = Mesh(mesh.devices.reshape(NX, NZHI, NCORE, NY, NZLO), ALL)
    in_specs = (P(ALL, None), P(ALL), P(ALL, None), P(ALL))
    return jax.shard_map(project, mesh=fine, in_specs=in_specs, out_specs=P(ALL, None, None), check_vma=False)
```
